16 devices in a mesh: data: 4 (over z, y), tp: 4 (over x, core).
Axes of the slice: x: 2, y: 2, z: 2, core: 2. Of those that a mesh axis runs over, the one named last changes fastest.
Arguments:
- x: bfloat16 [2048, 49152], P('data', 'tp'), parts along dimension 0
- w: bfloat16 [49152, 12288], P('tp')
Outputs:
- output: bfloat16 [2048, 12288], P('data'), parts along dimension 0
There are 4 independent parts. The reference program is written for one: setup_inputs(seed, part) draws one part's arguments, and reference() takes and returns one part's arrays. A program takes and returns all parts, laid end to end along the dimension named above; an argument that names none is the same for every part.
All inputs are finite; a program needn't handle non-finite values.
Results may differ from the reference program's by a relative error of at most 0.0103023.
Values are sent between devices in bfloat16 or wider.
A program may use at most 1.25 GiB of HBM per device.

```python
import jax
import jax.numpy as jnp

TOKENS = 512
D = 12288
FF = 49152


def setup_inputs(seed: int = 0, part: int = 0) -> dict:
    key = jax.random.key(seed)
    kx = jax.random.fold_in(jax.random.fold_in(key, 1), part)
    kw = jax.random.fold_in(key, 2)
    x = jax.random.normal(kx, (TOKENS, FF), jnp.float32)
    w = jax.random.normal(kw, (FF, D), jnp.float32) * (FF ** -0.5)
    return {"x": x.astype(jnp.bfloat16), "w": w.astype(jnp.bfloat16)}


def reference(x, w):
    y = jnp.dot(x, w, preferred_element_type=jnp.float32)
    return y.astype(jnp.bfloat16)
```

```python
import functools

import jax
import jax.numpy as jnp
from jax import lax
from jax.experimental import pallas as pl
from jax.experimental.pallas import tpu as pltpu
from jax.sharding import PartitionSpec as P

MESH = pl.DeviceIdType.MESH
BF16 = jnp.bfloat16
F32 = jnp.float32
HALF = 256
TILE = 2 * HALF
CHUNKS = 8
SLOTS = CHUNKS
LAG = 3
PIECE = 256


def fused(x, w, y, xv, wv, acc, own, pbuf, precv, sbuf, x_sem, w_sem, p_send, p_recv, s_send, s_recv, y_send, y_recv):
    rows, depth = x.shape
    tiles = w.shape[1] // TILE
    chunk = depth // CHUNKS
    pushes = chunk // HALF
    pieces = rows // PIECE
    me = lax.axis_index("tp")
    core = lax.rem(me, 2)
    partner = me + 1 - 2 * core
    across = lax.rem(me + 2, 4)

    def x_copy(q):
        cols = pl.ds(q * chunk, chunk)
        return pltpu.make_async_copy(x.at[:, cols], xv.at[:, cols], x_sem.at[q])

    def w_copies(t, q):
        deep = pl.ds(q * chunk, chunk)
        return [
            pltpu.make_async_copy(
                w.at[deep, pl.ds(pl.multiple_of(t * TILE + half * HALF, HALF), HALF)],
                wv.at[q, m],
                w_sem.at[q, m],
            )
            for m, half in enumerate((core, 1 - core))
        ]

    def p_copy(v):
        s = lax.rem(v, 2)
        return pltpu.make_async_remote_copy(
            src_ref=pbuf, dst_ref=precv.at[s], send_sem=p_send.at[s], recv_sem=p_recv.at[s],
            device_id={"tp": partner}, device_id_type=MESH,
        )

    def s_copy(v):
        s = lax.rem(v, 4)
        return pltpu.make_async_remote_copy(
            src_ref=sbuf.at[lax.rem(v, 2)], dst_ref=y.at[v + LAG, core], send_sem=s_send.at[s], recv_sem=s_recv.at[s],
            device_id={"tp": across}, device_id_type=MESH,
        )

    def y_copy(v):
        return pltpu.make_async_remote_copy(
            src_ref=y.at[v + LAG, core], dst_ref=y.at[v + LAG, core], send_sem=y_send.at[v], recv_sem=y_recv.at[v],
            device_id={"tp": partner}, device_id_type=MESH,
        )

    def sum_chip(v):
        sbuf[lax.rem(v, 2)] = (own[...] + precv[lax.rem(v, 2)].astype(F32)).astype(BF16)

    def sum_all(v):
        y[v + LAG, core] = (sbuf[lax.rem(v + 4, 2)].astype(F32) + y[v + LAG, core].astype(F32)).astype(BF16)

    def body():
        def pop(parity):
            own[...] = acc[parity, 0]
            pbuf[...] = acc[parity, 1].astype(BF16)

        for q in range(SLOTS - 1):
            x_copy(q).start()
            for c in w_copies(0, q):
                c.start()
        x_copy(CHUNKS - 1).start()

        barrier = pltpu.get_barrier_semaphore()
        for other in (partner, across):
            pl.semaphore_signal(barrier, inc=1, device_id={"tp": other}, device_id_type=MESH)
        pl.semaphore_wait(barrier, 2)

        x_copy(0).wait()
        for c in w_copies(0, 0):
            c.wait()

        def two_tiles(i, carry):
            for parity in range(2):
                t = 2 * i + parity
                for q in range(CHUNKS):
                    if q == CHUNKS - 1:
                        if parity == 0:
                            for c in w_copies(t + 1, 0):
                                c.wait()
                        else:
                            @pl.when(t + 1 < tiles)
                            def _():
                                for c in w_copies(t + 1, 0):
                                    c.wait()
                    else:
                        if parity == 0:
                            @pl.when(t == 0)
                            def _():
                                x_copy(q + 1).wait()
                        for c in w_copies(t, q + 1):
                            c.wait()
                    if q == 0:
                        for c in w_copies(t, CHUNKS - 1):
                            c.start()
                    elif parity == 0:
                        for c in w_copies(t + 1, q - 1):
                            c.start()
                    else:
                        @pl.when(t + 1 < tiles)
                        def _():
                            for c in w_copies(t + 1, q - 1):
                                c.start()
                    if q == 0:
                        @pl.when(t >= LAG)
                        def _():
                            s_copy(t - LAG).wait()
                    if q == 2:
                        @pl.when(t >= LAG)
                        def _():
                            y_copy(t - LAG).start()
                        @pl.when(t >= 1)
                        def _():
                            p_copy(t - 1).start()
                    if q == 4:
                        @pl.when(t >= 1)
                        def _():
                            p_copy(t - 1).wait()
                    if q == 5:
                        @pl.when(t >= 1)
                        def _():
                            s_copy(t - 1).start()

                    for m in range(2):
                        part = jnp.dot(xv[:, pl.ds(q * chunk, chunk)], wv[q, m], preferred_element_type=F32)
                        acc[parity, m] = part if q == 0 else acc[parity, m] + part
                    if q == 0:
                        sum_all(t - LAG)
                    if q == 1:
                        pop(1 - parity)
                    if q == 4:
                        sum_chip(t + 1)
            return carry

        lax.fori_loop(0, tiles // 2, two_tiles, 0)

        last = tiles - 1
        pop(last % 2)
        p_copy(last).start()
        s_copy(last - 2).wait()
        sum_all(last - 2)
        y_copy(last - 2).start()
        p_copy(last).wait()
        sum_chip(last)
        s_copy(last).start()
        for v in (last - 1, last):
            s_copy(v).wait()
            sum_all(v)
            y_copy(v).start()

        def finish(v, carry):
            y_copy(v).wait()
            return carry

        lax.fori_loop(0, tiles, finish, 0)

    body()


def place(y, out, sems):
    tiles = out.shape[1] // TILE
    copies = []
    for t in range(tiles):
        for h in range(2):
            copies.append(
                pltpu.make_async_copy(y.at[t + LAG, h], out.at[:, pl.ds(t * TILE + h * HALF, HALF)], sems.at[2 * t + h])
            )
    for c in copies:
        c.start()
    for c in copies:
        c.wait()


def solution(mesh):
    def local(x, w):
        rows, depth = x.shape
        columns = w.shape[1]
        tiles = columns // TILE
        chunk = depth // CHUNKS
        x = pltpu.with_memory_space_constraint(x, pltpu.HBM)
        w = pltpu.with_memory_space_constraint(w, pltpu.HBM)
        y = pl.pallas_call(
            fused,
            out_shape=pltpu.VMEM((tiles + LAG, 2, rows, HALF), BF16),
            in_specs=[pl.BlockSpec(memory_space=pl.ANY)] * 2,
            out_specs=pl.BlockSpec(memory_space=pltpu.VMEM),
            scratch_shapes=[
                pltpu.VMEM((rows, depth), BF16),
                pltpu.VMEM((SLOTS, 2, chunk, HALF), BF16),
                pltpu.VMEM((2, 2, rows, HALF), F32),
                pltpu.VMEM((rows, HALF), F32),
                pltpu.VMEM((rows, HALF), BF16),
                pltpu.VMEM((2, rows, HALF), BF16),
                pltpu.VMEM((2, rows, HALF), BF16),
                pltpu.SemaphoreType.DMA((CHUNKS,)),
                pltpu.SemaphoreType.DMA((SLOTS, 2)),
                pltpu.SemaphoreType.DMA((2,)),
                pltpu.SemaphoreType.DMA((2,)),
                pltpu.SemaphoreType.DMA((4,)),
                pltpu.SemaphoreType.DMA((4,)),
                pltpu.SemaphoreType.DMA((tiles,)),
                pltpu.SemaphoreType.DMA((tiles,)),
            ],
            compiler_params=pltpu.CompilerParams(
                collective_id=0, has_side_effects=True, vmem_limit_bytes=48 * 2**20
            ),
            name="fused",
        )(x, w)
        return pl.pallas_call(
            place,
            out_shape=jax.ShapeDtypeStruct((rows, columns), BF16),
            in_specs=[pl.BlockSpec(memory_space=pltpu.VMEM)],
            out_specs=pl.BlockSpec(memory_space=pl.ANY),
            scratch_shapes=[pltpu.SemaphoreType.DMA((2 * tiles,))],
            compiler_params=pltpu.CompilerParams(vmem_limit_bytes=16 * 2**20),
            name="place",
        )(y)

    return jax.shard_map(local, mesh=mesh, in_specs=(P("data", "tp"), P("tp", None)), out_specs=P("data", None), check_vma=False)
```

```python
import jax
import jax.numpy as jnp
from jax import lax
from jax.experimental import pallas as pl
from jax.experimental.pallas import tpu as pltpu
from jax.sharding import PartitionSpec as P

MESH = pl.DeviceIdType.MESH
BF16 = jnp.bfloat16
F32 = jnp.float32
HALF = 256
TILE = 2 * HALF
CHUNKS = 8
PIECE = 128
LAG = 3


def fused(x, w, y, xv, wv, acc, own, pbuf, precv, sbuf, x_sem, w0_sem, w_sem, p_send, p_recv, s_send, s_recv, y_send, y_recv):
    depth = x.shape[1]
    tiles = w.shape[1] // TILE
    chunk = depth // CHUNKS
    pieces = [pl.ds(r, PIECE) for r in range(0, x.shape[0], PIECE)]
    me = lax.axis_index("tp")
    core = lax.rem(me, 2)
    partner = me + 1 - 2 * core
    across = lax.rem(me + 2, 4)

    def columns(t, half):
        return pl.ds(pl.multiple_of(t * TILE + half * HALF, HALF), HALF)

    def own_ref(t):
        return wv.at[lax.rem(t, 2), :, pl.ds(HALF, HALF)]

    def other_ref(t):
        return wv.at[lax.rem(t + 1, 2), :, pl.ds(0, HALF)]

    def own_slab(t):
        return pltpu.make_async_copy(w.at[:, columns(t, core)], own_ref(t), w_sem.at[1, lax.rem(t, 2)])

    def other_slab(t):
        return pltpu.make_async_copy(w.at[:, columns(t, 1 - core)], other_ref(t), w_sem.at[0, lax.rem(t, 2)])

    def x_copy(q):
        cols = pl.ds(pl.multiple_of(q * chunk, chunk), chunk)
        return pltpu.make_async_copy(x.at[:, cols], xv.at[:, cols], x_sem.at[q])

    def first_copies(q):
        deep = pl.ds(pl.multiple_of(q * chunk, chunk), chunk)
        return [
            pltpu.make_async_copy(w.at[deep, columns(0, 1 - core)], wv.at[1, deep, pl.ds(0, HALF)], w0_sem.at[0, q]),
            pltpu.make_async_copy(w.at[deep, columns(0, core)], wv.at[0, deep, pl.ds(HALF, HALF)], w0_sem.at[1, q]),
        ]

    def p_copy(v):
        s = lax.rem(v, 2)
        return pltpu.make_async_remote_copy(
            src_ref=pbuf.at[s], dst_ref=precv.at[s], send_sem=p_send.at[s], recv_sem=p_recv.at[s],
            device_id={"tp": partner}, device_id_type=MESH,
        )

    def s_copy(v):
        s = lax.rem(v, 4)
        return pltpu.make_async_remote_copy(
            src_ref=sbuf.at[s], dst_ref=y.at[v + LAG, core], send_sem=s_send.at[v], recv_sem=s_recv.at[v],
            device_id={"tp": across}, device_id_type=MESH,
        )

    def y_copy(v):
        return pltpu.make_async_remote_copy(
            src_ref=y.at[v + LAG, core], dst_ref=y.at[v + LAG, core], send_sem=y_send.at[v], recv_sem=y_recv.at[v],
            device_id={"tp": partner}, device_id_type=MESH,
        )

    def sum_chip(v):
        for at in pieces:
            sbuf[lax.rem(v, 4), at] = own[at] + precv[lax.rem(v, 2), at]

    def sum_all(v):
        for at in pieces:
            y[v + LAG, core, at] = sbuf[lax.rem(v + 4, 4), at] + y[v + LAG, core, at]

    def product(weights):
        return jnp.dot(xv[...], weights[...], preferred_element_type=F32).astype(BF16)

    for q in range(CHUNKS):
        x_copy(q).start()
        for c in first_copies(q):
            c.start()
    other_slab(1).start()
    own_slab(1).start()

    barrier = pltpu.get_barrier_semaphore()
    for other in (partner, across):
        pl.semaphore_signal(barrier, inc=1, device_id={"tp": other}, device_id_type=MESH)
    pl.semaphore_wait(barrier, 2)

    acc[...] = jnp.zeros_like(acc)

    def piece_of_depth(q, carry):
        x_copy(q).wait()
        for c in first_copies(q):
            c.wait()
        deep = pl.ds(pl.multiple_of(q * chunk, chunk), chunk)
        weights = jnp.concatenate([wv[1, deep, pl.ds(0, HALF)], wv[0, deep, pl.ds(HALF, HALF)]], axis=1)
        acc[...] += jnp.dot(xv[:, deep], weights, preferred_element_type=F32)
        return carry

    lax.fori_loop(0, CHUNKS, piece_of_depth, 0)
    for at in pieces:
        pbuf[0, at] = acc[at, :HALF].astype(BF16)
        own[at] = acc[at, HALF:].astype(BF16)

    other_slab(2).start()
    p_copy(0).start()
    other_slab(1).wait()
    pbuf[1] = product(other_ref(1))

    def fence(t):
        p_copy(t - 1).wait()

        @pl.when(t >= LAG)
        def _():
            s_copy(t - LAG).wait()

        sum_chip(t - 1)
        s_copy(t - 1).start()
        p_copy(t).start()

        @pl.when(t >= LAG + 1)
        def _():
            y_copy(t - LAG - 1).start()

    def tile(t, carry):
        own_slab(t + 1).start()

        @pl.when(t + 2 < tiles)
        def _():
            other_slab(t + 2).start()

        fence(t)
        own_slab(t).wait()
        other_slab(t + 1).wait()
        both = product(wv.at[lax.rem(t, 2)])
        pbuf[lax.rem(t + 1, 2)] = both[:, :HALF]
        own[...] = both[:, HALF:]
        sum_all(t - LAG)
        return carry

    last = tiles - 1
    lax.fori_loop(1, last - 1, tile, 0)

    own_slab(last).start()
    fence(last - 1)
    own_slab(last - 1).wait()
    own[...] = product(own_ref(last - 1))
    sum_all(last - 1 - LAG)

    p_copy(last - 1).wait()
    sum_chip(last - 1)
    s_copy(last - 1).start()
    s_copy(last - 3).wait()
    y_copy(last - 4).start()
    other_slab(last).wait()
    pbuf[lax.rem(last, 2)] = product(other_ref(last))
    sum_all(last - 3)

    p_copy(last).start()
    y_copy(last - 3).start()
    own_slab(last).wait()
    own[...] = product(own_ref(last))

    p_copy(last).wait()
    sum_chip(last)
    s_copy(last).start()
    for v in (last - 2, last - 1, last):
        s_copy(v).wait()
        sum_all(v)
        y_copy(v).start()

    def finish(v, carry):
        y_copy(v).wait()
        return carry

    lax.fori_loop(0, tiles, finish, 0)


def place(y, out, sems):
    tiles = out.shape[1] // TILE
    copies = []
    for t in range(tiles):
        for h in range(2):
            copies.append(
                pltpu.make_async_copy(y.at[t + LAG, h], out.at[:, pl.ds(t * TILE + h * HALF, HALF)], sems.at[2 * t + h])
            )
    for c in copies:
        c.start()
    for c in copies:
        c.wait()


def solution(mesh):
    def local(x, w):
        rows, depth = x.shape
        columns = w.shape[1]
        tiles = columns // TILE
        x = pltpu.with_memory_space_constraint(x, pltpu.HBM)
        w = pltpu.with_memory_space_constraint(w, pltpu.HBM)
        y = pl.pallas_call(
            fused,
            out_shape=pltpu.VMEM((tiles + LAG, 2, rows, HALF), BF16),
            in_specs=[pl.BlockSpec(memory_space=pl.ANY)] * 2,
            out_specs=pl.BlockSpec(memory_space=pltpu.VMEM),
            scratch_shapes=[
                pltpu.VMEM((rows, depth), BF16),
                pltpu.VMEM((2, depth, TILE), BF16),
                pltpu.VMEM((rows, TILE), F32),
                pltpu.VMEM((rows, HALF), BF16),
                pltpu.VMEM((2, rows, HALF), BF16),
                pltpu.VMEM((2, rows, HALF), BF16),
                pltpu.VMEM((4, rows, HALF), BF16),
                pltpu.SemaphoreType.DMA((CHUNKS,)),
                pltpu.SemaphoreType.DMA((2, CHUNKS)),
                pltpu.SemaphoreType.DMA((2, 2)),
                pltpu.SemaphoreType.DMA((2,)),
                pltpu.SemaphoreType.DMA((2,)),
                pltpu.SemaphoreType.DMA((tiles,)),
                pltpu.SemaphoreType.DMA((tiles,)),
                pltpu.SemaphoreType.DMA((tiles,)),
                pltpu.SemaphoreType.DMA((tiles,)),
            ],
            compiler_params=pltpu.CompilerParams(
                collective_id=0, has_side_effects=True, vmem_limit_bytes=48 * 2**20
            ),
            name="fused",
        )(x, w)
        return pl.pallas_call(
            place,
            out_shape=jax.ShapeDtypeStruct((rows, columns), BF16),
            in_specs=[pl.BlockSpec(memory_space=pltpu.VMEM)],
            out_specs=pl.BlockSpec(memory_space=pl.ANY),
            scratch_shapes=[pltpu.SemaphoreType.DMA((2 * tiles,))],
            compiler_params=pltpu.CompilerParams(vmem_limit_bytes=16 * 2**20),
            name="place",
        )(y)

    return jax.shard_map(local, mesh=mesh, in_specs=(P("data", "tp"), P("tp", None)), out_specs=P("data", None), check_vma=False)
```

```python
import jax
import jax.numpy as jnp
from jax import lax
from jax.experimental import pallas as pl
from jax.experimental.pallas import tpu as pltpu
from jax.sharding import PartitionSpec as P

MESH = pl.DeviceIdType.MESH
BF16 = jnp.bfloat16
F32 = jnp.float32
HALF = 256
TILE = 2 * HALF
CHUNKS = 8
PIECE = 128
AHEAD = 3
SPLIT = 4
LAG = 3


def fused(x, w, y, xv, wv, acc, own, pbuf, precv, sbuf, x_sem, w0_sem, w_sem, p_send, p_recv, s_send, s_recv, y_send, y_recv):
    depth = x.shape[1]
    tiles = w.shape[1] // TILE
    chunk = depth // CHUNKS
    rows = x.shape[0]
    middle, shallow = rows // 2, depth // 2
    last = tiles - 1
    pieces = [pl.ds(r, PIECE) for r in range(0, rows, PIECE)]
    half_rows = [pl.ds(0, middle), pl.ds(middle, middle)]
    me = lax.axis_index("tp")
    core = lax.rem(me, 2)
    partner = me + 1 - 2 * core
    across = lax.rem(me + 2, 4)

    def columns(t, half):
        return pl.ds(pl.multiple_of(t * TILE + half * HALF, HALF), HALF)

    def own_ref(t):
        return wv.at[lax.rem(t, 2), :, pl.ds(HALF, HALF)]

    def other_ref(t):
        return wv.at[lax.rem(t + 1, 2), :, pl.ds(0, HALF)]

    def own_slab(t):
        return pltpu.make_async_copy(w.at[:, columns(t, core)], own_ref(t), w_sem.at[1, lax.rem(t, 2)])

    def other_slab(t):
        return pltpu.make_async_copy(w.at[:, columns(t, 1 - core)], other_ref(t), w_sem.at[0, lax.rem(t, 2)])

    def x_copy(q):
        cols = pl.ds(pl.multiple_of(q * chunk, chunk), chunk)
        return pltpu.make_async_copy(x.at[:, cols], xv.at[:, cols], x_sem.at[q])

    def first_copies(q):
        deep = pl.ds(pl.multiple_of(q * chunk, chunk), chunk)
        return [
            pltpu.make_async_copy(w.at[deep, columns(0, 1 - core)], wv.at[1, deep, pl.ds(0, HALF)], w0_sem.at[0, q]),
            pltpu.make_async_copy(w.at[deep, columns(0, core)], wv.at[0, deep, pl.ds(HALF, HALF)], w0_sem.at[1, q]),
        ]

    def p_copy(v):
        s = lax.rem(v, 2)
        return pltpu.make_async_remote_copy(
            src_ref=pbuf.at[s], dst_ref=precv.at[s], send_sem=p_send.at[s], recv_sem=p_recv.at[s],
            device_id={"tp": partner}, device_id_type=MESH,
        )

    def s_copy(v, h):
        s = lax.rem(v, 4)
        return pltpu.make_async_remote_copy(
            src_ref=sbuf.at[s, half_rows[h]], dst_ref=y.at[v + LAG, core, half_rows[h]],
            send_sem=s_send.at[v, h], recv_sem=s_recv.at[v, h],
            device_id={"tp": across}, device_id_type=MESH,
        )

    def s_wait(v):
        for h in range(2):
            s_copy(v, h).wait()

    def y_copy(v):
        return pltpu.make_async_remote_copy(
            src_ref=y.at[v + LAG, core], dst_ref=y.at[v + LAG, core], send_sem=y_send.at[v], recv_sem=y_recv.at[v],
            device_id={"tp": partner}, device_id_type=MESH,
        )

    def y_last(h):
        return pltpu.make_async_remote_copy(
            src_ref=y.at[last + LAG, core, half_rows[h]], dst_ref=y.at[last + LAG, core, half_rows[h]],
            send_sem=y_send.at[last + h], recv_sem=y_recv.at[last + h],
            device_id={"tp": partner}, device_id_type=MESH,
        )

    def send_chip(v, h):
        for at in pieces[h * len(pieces) // 2 : (h + 1) * len(pieces) // 2]:
            sbuf[lax.rem(v, 4), at] = own[at] + precv[lax.rem(v, 2), at]
        s_copy(v, h).start()

    def sum_all(v, which=pieces):
        for at in which:
            y[v + LAG, core, at] = sbuf[lax.rem(v + 4, 4), at] + y[v + LAG, core, at]

    def dot(a, b):
        return jnp.dot(a, b, preferred_element_type=F32)

    def other_product(t):
        weights = other_ref(t)[...]
        slot = lax.rem(t, 2)
        halves = [dot(xv[at], weights).astype(BF16) for at in half_rows]
        for at, half in zip(half_rows, halves):
            pbuf[slot, at] = half

    def own_product(t, h):
        near, far = pl.ds(0, shallow), pl.ds(shallow, shallow)
        cols = pl.ds(HALF, HALF)
        first = dot(xv[half_rows[h], near], wv[lax.rem(t, 2), near, cols])
        second = dot(xv[half_rows[h], far], wv[lax.rem(t, 2), far, cols])
        own[half_rows[h]] = (first + second).astype(BF16)

    def first_start(q):
        x_copy(q).start()
        for c in first_copies(q):
            c.start()

    for q in range(AHEAD):
        first_start(q)

    barrier = pltpu.get_barrier_semaphore()
    for other in (partner, across):
        pl.semaphore_signal(barrier, inc=1, device_id={"tp": other}, device_id_type=MESH)
    pl.semaphore_wait(barrier, 2)

    acc[...] = jnp.zeros_like(acc)

    def piece_of_depth(q, carry):
        x_copy(q).wait()
        for c in first_copies(q):
            c.wait()

        @pl.when(q + AHEAD < CHUNKS)
        def _():
            first_start(q + AHEAD)

        @pl.when(q == CHUNKS - AHEAD)
        def _():
            other_slab(1).start()

        @pl.when(q == CHUNKS - 1)
        def _():
            own_slab(1).start()

        deep = pl.ds(pl.multiple_of(q * chunk, chunk), chunk)
        weights = jnp.concatenate([wv[1, deep, pl.ds(0, HALF)], wv[0, deep, pl.ds(HALF, HALF)]], axis=1)
        acc[...] += jnp.dot(xv[:, deep], weights, preferred_element_type=F32)
        return carry

    lax.fori_loop(0, CHUNKS, piece_of_depth, 0)
    for at in pieces:
        pbuf[0, at] = acc[at, :HALF].astype(BF16)
        own[at] = acc[at, HALF:].astype(BF16)

    other_slab(2).start()
    p_copy(0).start()
    other_slab(1).wait()
    other_product(1)

    def fence(t):
        p_copy(t - 1).wait()

        @pl.when(t >= LAG)
        def _():
            s_wait(t - LAG)

        send_chip(t - 1, 0)
        send_chip(t - 1, 1)
        p_copy(t).start()

        @pl.when(t >= LAG + 1)
        def _():
            y_copy(t - LAG - 1).start()

    def next_slabs(t):
        own_slab(t + 1).start()

        @pl.when(t + 2 < tiles)
        def _():
            other_slab(t + 2).start()

    def tile(t, carry):
        next_slabs(t)
        fence(t)
        own_slab(t).wait()
        other_slab(t + 1).wait()
        both = dot(xv[...], wv[lax.rem(t, 2)]).astype(BF16)
        pbuf[lax.rem(t + 1, 2)] = both[:, :HALF]
        own[...] = both[:, HALF:]
        sum_all(t - LAG)
        return carry

    def own_halves(t):
        own_slab(t).wait()
        own_product(t, 0)
        sum_all(t - LAG)
        p_copy(t).wait()
        send_chip(t, 0)
        own_product(t, 1)
        send_chip(t, 1)

    def split_tile(t, carry):
        next_slabs(t)
        own_halves(t)
        s_wait(t - 2)
        other_slab(t + 1).wait()
        other_product(t + 1)
        p_copy(t + 1).start()
        y_copy(t - LAG).start()
        return carry

    lax.fori_loop(1, tiles - SPLIT, tile, 0)
    fence(tiles - SPLIT)
    lax.fori_loop(tiles - SPLIT, last, split_tile, 0)
    own_halves(last)

    y_copy(last - LAG).start()
    for v in (last - 2, last - 1):
        s_wait(v)
        sum_all(v)
        y_copy(v).start()
    for h in range(2):
        s_copy(last, h).wait()
        sum_all(last, pieces[h * len(pieces) // 2 : (h + 1) * len(pieces) // 2])
        y_last(h).start()

    def finish(v, carry):
        y_copy(v).wait()
        return carry

    lax.fori_loop(0, last, finish, 0)
    for h in range(2):
        y_last(h).wait()


def place(y, out, sems):
    tiles = out.shape[1] // TILE
    copies = []
    for t in range(tiles):
        for h in range(2):
            copies.append(
                pltpu.make_async_copy(y.at[t + LAG, h], out.at[:, pl.ds(t * TILE + h * HALF, HALF)], sems.at[2 * t + h])
            )
    for c in copies:
        c.start()
    for c in copies:
        c.wait()


def solution(mesh):
    def local(x, w):
        rows, depth = x.shape
        columns = w.shape[1]
        tiles = columns // TILE
        x = pltpu.with_memory_space_constraint(x, pltpu.HBM)
        w = pltpu.with_memory_space_constraint(w, pltpu.HBM)
        y = pl.pallas_call(
            fused,
            out_shape=pltpu.VMEM((tiles + LAG, 2, rows, HALF), BF16),
            in_specs=[pl.BlockSpec(memory_space=pl.ANY)] * 2,
            out_specs=pl.BlockSpec(memory_space=pltpu.VMEM),
            scratch_shapes=[
                pltpu.VMEM((rows, depth), BF16),
                pltpu.VMEM((2, depth, TILE), BF16),
                pltpu.VMEM((rows, TILE), F32),
                pltpu.VMEM((rows, HALF), BF16),
                pltpu.VMEM((2, rows, HALF), BF16),
                pltpu.VMEM((2, rows, HALF), BF16),
                pltpu.VMEM((4, rows, HALF), BF16),
                pltpu.SemaphoreType.DMA((CHUNKS,)),
                pltpu.SemaphoreType.DMA((2, CHUNKS)),
                pltpu.SemaphoreType.DMA((2, 2)),
                pltpu.SemaphoreType.DMA((2,)),
                pltpu.SemaphoreType.DMA((2,)),
                pltpu.SemaphoreType.DMA((tiles, 2)),
                pltpu.SemaphoreType.DMA((tiles, 2)),
                pltpu.SemaphoreType.DMA((tiles + 1,)),
                pltpu.SemaphoreType.DMA((tiles + 1,)),
            ],
            compiler_params=pltpu.CompilerParams(
                collective_id=0, has_side_effects=True, vmem_limit_bytes=48 * 2**20
            ),
            name="fused",
        )(x, w)
        return pl.pallas_call(
            place,
            out_shape=jax.ShapeDtypeStruct((rows, columns), BF16),
            in_specs=[pl.BlockSpec(memory_space=pltpu.VMEM)],
            out_specs=pl.BlockSpec(memory_space=pl.ANY),
            scratch_shapes=[pltpu.SemaphoreType.DMA((2 * tiles,))],
            compiler_params=pltpu.CompilerParams(vmem_limit_bytes=16 * 2**20),
            name="place",
        )(y)

    return jax.shard_map(local, mesh=mesh, in_specs=(P("data", "tp"), P("tp", None)), out_specs=P("data", None), check_vma=False)
```

```python
import jax
import jax.numpy as jnp
from jax import lax
from jax.experimental import pallas as pl
from jax.experimental.pallas import tpu as pltpu
from jax.sharding import PartitionSpec as P

MESH = pl.DeviceIdType.MESH
BF16 = jnp.bfloat16
F32 = jnp.float32
HALF = 256
TILE = 2 * HALF
CHUNKS = 8
PIECE = 128
AHEAD = 3
SPLIT = 4
LAG = 3


def fused(x, w, y, xv, wv, acc, own, pbuf, precv, sbuf, x_sem, w0_sem, w_sem, p_send, p_recv, s_send, s_recv, y_send, y_recv):
    depth = x.shape[1]
    tiles = w.shape[1] // TILE
    chunk = depth // CHUNKS
    rows = x.shape[0]
    middle, shallow = rows // 2, depth // 2
    last = tiles - 1
    pieces = [pl.ds(r, PIECE) for r in range(0, rows, PIECE)]
    half_rows = [pl.ds(0, middle), pl.ds(middle, middle)]
    me = lax.axis_index("tp")
    core = lax.rem(me, 2)
    partner = me + 1 - 2 * core
    across = lax.rem(me + 2, 4)

    def columns(t, half):
        return pl.ds(pl.multiple_of(t * TILE + half * HALF, HALF), HALF)

    def own_ref(t):
        return wv.at[lax.rem(t, 2), :, pl.ds(HALF, HALF)]

    def other_ref(t):
        return wv.at[lax.rem(t + 1, 2), :, pl.ds(0, HALF)]

    def own_slab(t):
        return pltpu.make_async_copy(w.at[:, columns(t, core)], own_ref(t), w_sem.at[1, lax.rem(t, 2)])

    def other_slab(t):
        return pltpu.make_async_copy(w.at[:, columns(t, 1 - core)], other_ref(t), w_sem.at[0, lax.rem(t, 2)])

    def x_copy(q):
        cols = pl.ds(pl.multiple_of(q * chunk, chunk), chunk)
        return pltpu.make_async_copy(x.at[:, cols], xv.at[:, cols], x_sem.at[q])

    def first_copies(q):
        deep = pl.ds(pl.multiple_of(q * chunk, chunk), chunk)
        return [
            pltpu.make_async_copy(w.at[deep, columns(0, 1 - core)], wv.at[1, deep, pl.ds(0, HALF)], w0_sem.at[0, q]),
            pltpu.make_async_copy(w.at[deep, columns(0, core)], wv.at[0, deep, pl.ds(HALF, HALF)], w0_sem.at[1, q]),
        ]

    def p_copy(v):
        s = lax.rem(v, 2)
        return pltpu.make_async_remote_copy(
            src_ref=pbuf.at[s], dst_ref=precv.at[s], send_sem=p_send.at[s], recv_sem=p_recv.at[s],
            device_id={"tp": partner}, device_id_type=MESH,
        )

    def s_copy(v, h):
        s = lax.rem(v, 4)
        return pltpu.make_async_remote_copy(
            src_ref=sbuf.at[s, half_rows[h]], dst_ref=y.at[v + LAG, core, half_rows[h]],
            send_sem=s_send.at[v, h], recv_sem=s_recv.at[v, h],
            device_id={"tp": across}, device_id_type=MESH,
        )

    def s_wait(v):
        for h in range(2):
            s_copy(v, h).wait()

    def y_copy(v):
        return pltpu.make_async_remote_copy(
            src_ref=y.at[v + LAG, core], dst_ref=y.at[v + LAG, core], send_sem=y_send.at[v], recv_sem=y_recv.at[v],
            device_id={"tp": partner}, device_id_type=MESH,
        )

    def y_last(h):
        return pltpu.make_async_remote_copy(
            src_ref=y.at[last + LAG, core, half_rows[h]], dst_ref=y.at[last + LAG, core, half_rows[h]],
            send_sem=y_send.at[last + h], recv_sem=y_recv.at[last + h],
            device_id={"tp": partner}, device_id_type=MESH,
        )

    def send_chip(v, h):
        for at in pieces[h * len(pieces) // 2 : (h + 1) * len(pieces) // 2]:
            sbuf[lax.rem(v, 4), at] = own[at] + precv[lax.rem(v, 2), at]
        s_copy(v, h).start()

    def sum_all(v, which=pieces):
        for at in which:
            y[v + LAG, core, at] = sbuf[lax.rem(v + 4, 4), at] + y[v + LAG, core, at]

    def dot(a, b):
        return jnp.dot(a, b, preferred_element_type=F32)

    def other_product(t):
        weights = other_ref(t)[...]
        slot = lax.rem(t, 2)
        halves = [dot(xv[at], weights).astype(BF16) for at in half_rows]
        for at, half in zip(half_rows, halves):
            pbuf[slot, at] = half

    def own_product(t, h):
        near, far = pl.ds(0, shallow), pl.ds(shallow, shallow)
        cols = pl.ds(HALF, HALF)
        weights = wv.at[lax.rem(t, 2), :, cols]
        acc[half_rows[h], :HALF] = dot(xv[half_rows[h], near], weights[near])
        second = dot(xv[half_rows[h], far], weights[far])
        own[half_rows[h]] = (acc[half_rows[h], :HALF] + second).astype(BF16)

    def first_start(q):
        x_copy(q).start()
        for c in first_copies(q):
            c.start()

    for q in range(AHEAD):
        first_start(q)

    barrier = pltpu.get_barrier_semaphore()
    for other in (partner, across):
        pl.semaphore_signal(barrier, inc=1, device_id={"tp": other}, device_id_type=MESH)
    pl.semaphore_wait(barrier, 2)

    acc[...] = jnp.zeros_like(acc)

    def piece_of_depth(q, carry):
        x_copy(q).wait()
        for c in first_copies(q):
            c.wait()

        @pl.when(q + AHEAD < CHUNKS)
        def _():
            first_start(q + AHEAD)

        @pl.when(q == CHUNKS - AHEAD)
        def _():
            other_slab(1).start()

        @pl.when(q == CHUNKS - 1)
        def _():
            own_slab(1).start()

        deep = pl.ds(pl.multiple_of(q * chunk, chunk), chunk)
        weights = jnp.concatenate([wv[1, deep, pl.ds(0, HALF)], wv[0, deep, pl.ds(HALF, HALF)]], axis=1)
        acc[...] += jnp.dot(xv[:, deep], weights, preferred_element_type=F32)
        return carry

    lax.fori_loop(0, CHUNKS, piece_of_depth, 0)
    for at in pieces:
        pbuf[0, at] = acc[at, :HALF].astype(BF16)
        own[at] = acc[at, HALF:].astype(BF16)

    other_slab(2).start()
    p_copy(0).start()
    other_slab(1).wait()
    other_product(1)

    def fence(t):
        p_copy(t - 1).wait()

        @pl.when(t >= LAG)
        def _():
            s_wait(t - LAG)

        send_chip(t - 1, 0)
        send_chip(t - 1, 1)
        p_copy(t).start()

        @pl.when(t >= LAG + 1)
        def _():
            y_copy(t - LAG - 1).start()

    def next_slabs(t):
        own_slab(t + 1).start()

        @pl.when(t + 2 < tiles)
        def _():
            other_slab(t + 2).start()

    def tile(t, carry):
        next_slabs(t)
        fence(t)
        own_slab(t).wait()
        other_slab(t + 1).wait()
        both = dot(xv[...], wv[lax.rem(t, 2)]).astype(BF16)
        pbuf[lax.rem(t + 1, 2)] = both[:, :HALF]
        own[...] = both[:, HALF:]
        sum_all(t - LAG)
        return carry

    def own_halves(t):
        own_slab(t).wait()
        own_product(t, 0)
        sum_all(t - LAG)
        p_copy(t).wait()
        send_chip(t, 0)
        own_product(t, 1)
        send_chip(t, 1)

    def split_tile(t, carry):
        next_slabs(t)
        own_halves(t)
        s_wait(t - 2)
        other_slab(t + 1).wait()
        other_product(t + 1)
        p_copy(t + 1).start()
        y_copy(t - LAG).start()
        return carry

    lax.fori_loop(1, tiles - SPLIT, tile, 0)
    fence(tiles - SPLIT)
    lax.fori_loop(tiles - SPLIT, last, split_tile, 0)
    own_halves(last)

    y_copy(last - LAG).start()
    for v in (last - 2, last - 1):
        s_wait(v)
        sum_all(v)
        y_copy(v).start()
    for h in range(2):
        s_copy(last, h).wait()
        sum_all(last, pieces[h * len(pieces) // 2 : (h + 1) * len(pieces) // 2])
        y_last(h).start()

    def finish(v, carry):
        y_copy(v).wait()
        return carry

    lax.fori_loop(0, last, finish, 0)
    for h in range(2):
        y_last(h).wait()


def place(y, out, sems):
    tiles = out.shape[1] // TILE
    copies = []
    for t in range(tiles):
        for h in range(2):
            copies.append(
                pltpu.make_async_copy(y.at[t + LAG, h], out.at[:, pl.ds(t * TILE + h * HALF, HALF)], sems.at[2 * t + h])
            )
    for c in copies:
        c.start()
    for c in copies:
        c.wait()


def solution(mesh):
    def local(x, w):
        rows, depth = x.shape
        columns = w.shape[1]
        tiles = columns // TILE
        x = pltpu.with_memory_space_constraint(x, pltpu.HBM)
        w = pltpu.with_memory_space_constraint(w, pltpu.HBM)
        y = pl.pallas_call(
            fused,
            out_shape=pltpu.VMEM((tiles + LAG, 2, rows, HALF), BF16),
            in_specs=[pl.BlockSpec(memory_space=pl.ANY)] * 2,
            out_specs=pl.BlockSpec(memory_space=pltpu.VMEM),
            scratch_shapes=[
                pltpu.VMEM((rows, depth), BF16),
                pltpu.VMEM((2, depth, TILE), BF16),
                pltpu.VMEM((rows, TILE), F32),
                pltpu.VMEM((rows, HALF), BF16),
                pltpu.VMEM((2, rows, HALF), BF16),
                pltpu.VMEM((2, rows, HALF), BF16),
                pltpu.VMEM((4, rows, HALF), BF16),
                pltpu.SemaphoreType.DMA((CHUNKS,)),
                pltpu.SemaphoreType.DMA((2, CHUNKS)),
                pltpu.SemaphoreType.DMA((2, 2)),
                pltpu.SemaphoreType.DMA((2,)),
                pltpu.SemaphoreType.DMA((2,)),
                pltpu.SemaphoreType.DMA((tiles, 2)),
                pltpu.SemaphoreType.DMA((tiles, 2)),
                pltpu.SemaphoreType.DMA((tiles + 1,)),
                pltpu.SemaphoreType.DMA((tiles + 1,)),
            ],
            compiler_params=pltpu.CompilerParams(
                collective_id=0, has_side_effects=True, vmem_limit_bytes=48 * 2**20
            ),
            name="fused",
        )(x, w)
        return pl.pallas_call(
            place,
            out_shape=jax.ShapeDtypeStruct((rows, columns), BF16),
            in_specs=[pl.BlockSpec(memory_space=pltpu.VMEM)],
            out_specs=pl.BlockSpec(memory_space=pl.ANY),
            scratch_shapes=[pltpu.SemaphoreType.DMA((2 * tiles,))],
            compiler_params=pltpu.CompilerParams(vmem_limit_bytes=16 * 2**20),
            name="place",
        )(y)

    return jax.shard_map(local, mesh=mesh, in_specs=(P("data", "tp"), P("tp", None)), out_specs=P("data", None), check_vma=False)
```

```python
import jax
import jax.numpy as jnp
from jax import lax
from jax.experimental import pallas as pl
from jax.experimental.pallas import tpu as pltpu
from jax.sharding import PartitionSpec as P

MESH = pl.DeviceIdType.MESH
BF16 = jnp.bfloat16
F32 = jnp.float32
HALF = 256
TILE = 2 * HALF
CHUNKS = 8
PIECE = 128
AHEAD = 4
SPLIT = 5
LAG = 3


def fused(x, w, y, xv, wv, acc, own, pbuf, precv, sbuf, x_sem, w0_sem, w_sem, p_send, p_recv, s_send, s_recv, y_send, y_recv):
    depth = x.shape[1]
    tiles = w.shape[1] // TILE
    chunk = depth // CHUNKS
    rows = x.shape[0]
    middle, shallow = rows // 2, depth // 2
    last = tiles - 1
    pieces = [pl.ds(r, PIECE) for r in range(0, rows, PIECE)]
    half_rows = [pl.ds(0, middle), pl.ds(middle, middle)]
    me = lax.axis_index("tp")
    core = lax.rem(me, 2)
    partner = me + 1 - 2 * core
    across = lax.rem(me + 2, 4)

    def columns(t, half):
        return pl.ds(pl.multiple_of(t * TILE + half * HALF, HALF), HALF)

    def own_ref(t):
        return wv.at[lax.rem(t, 2), :, pl.ds(HALF, HALF)]

    def other_ref(t):
        return wv.at[lax.rem(t + 1, 2), :, pl.ds(0, HALF)]

    def own_slab(t):
        return pltpu.make_async_copy(w.at[:, columns(t, core)], own_ref(t), w_sem.at[1, lax.rem(t, 2)])

    def other_slab(t):
        return pltpu.make_async_copy(w.at[:, columns(t, 1 - core)], other_ref(t), w_sem.at[0, lax.rem(t, 2)])

    def x_copy(q):
        cols = pl.ds(pl.multiple_of(q * chunk, chunk), chunk)
        return pltpu.make_async_copy(x.at[:, cols], xv.at[:, cols], x_sem.at[q])

    def first_copies(q):
        deep = pl.ds(pl.multiple_of(q * chunk, chunk), chunk)
        return [
            pltpu.make_async_copy(w.at[deep, columns(0, 1 - core)], wv.at[1, deep, pl.ds(0, HALF)], w0_sem.at[0, q]),
            pltpu.make_async_copy(w.at[deep, columns(0, core)], wv.at[0, deep, pl.ds(HALF, HALF)], w0_sem.at[1, q]),
        ]

    def p_copy(v):
        s = lax.rem(v, 2)
        return pltpu.make_async_remote_copy(
            src_ref=pbuf.at[s], dst_ref=precv.at[s], send_sem=p_send.at[s], recv_sem=p_recv.at[s],
            device_id={"tp": partner}, device_id_type=MESH,
        )

    def s_copy(v, h):
        s = lax.rem(v, 4)
        return pltpu.make_async_remote_copy(
            src_ref=sbuf.at[s, half_rows[h]], dst_ref=y.at[v + LAG, core, half_rows[h]],
            send_sem=s_send.at[v, h], recv_sem=s_recv.at[v, h],
            device_id={"tp": across}, device_id_type=MESH,
        )

    def s_wait(v):
        for h in range(2):
            s_copy(v, h).wait()

    def y_copy(v):
        return pltpu.make_async_remote_copy(
            src_ref=y.at[v + LAG, core], dst_ref=y.at[v + LAG, core], send_sem=y_send.at[v], recv_sem=y_recv.at[v],
            device_id={"tp": partner}, device_id_type=MESH,
        )

    def y_last(h):
        return pltpu.make_async_remote_copy(
            src_ref=y.at[last + LAG, core, half_rows[h]], dst_ref=y.at[last + LAG, core, half_rows[h]],
            send_sem=y_send.at[last + h], recv_sem=y_recv.at[last + h],
            device_id={"tp": partner}, device_id_type=MESH,
        )

    def send_chip(v, h):
        for at in pieces[h * len(pieces) // 2 : (h + 1) * len(pieces) // 2]:
            sbuf[lax.rem(v, 4), at] = own[at] + precv[lax.rem(v, 2), at]
        s_copy(v, h).start()

    def sum_all(v, which=pieces):
        for at in which:
            y[v + LAG, core, at] = sbuf[lax.rem(v + 4, 4), at] + y[v + LAG, core, at]

    def dot(a, b):
        return jnp.dot(a, b, preferred_element_type=F32)

    def other_product(t):
        weights = other_ref(t)[...]
        slot = lax.rem(t, 2)
        halves = [dot(xv[at], weights).astype(BF16) for at in half_rows]
        for at, half in zip(half_rows, halves):
            pbuf[slot, at] = half

    def own_product(t, h):
        near, far = pl.ds(0, shallow), pl.ds(shallow, shallow)
        cols = pl.ds(HALF, HALF)
        weights = wv.at[lax.rem(t, 2), :, cols]
        acc[half_rows[h], :HALF] = dot(xv[half_rows[h], near], weights[near])
        second = dot(xv[half_rows[h], far], weights[far])
        own[half_rows[h]] = (acc[half_rows[h], :HALF] + second).astype(BF16)

    def first_start(q):
        x_copy(q).start()
        for c in first_copies(q):
            c.start()

    for q in range(AHEAD):
        first_start(q)

    barrier = pltpu.get_barrier_semaphore()
    for other in (partner, across):
        pl.semaphore_signal(barrier, inc=1, device_id={"tp": other}, device_id_type=MESH)
    pl.semaphore_wait(barrier, 2)

    acc[...] = jnp.zeros_like(acc)

    def piece_of_depth(q, carry):
        x_copy(q).wait()
        for c in first_copies(q):
            c.wait()

        @pl.when(q + AHEAD < CHUNKS)
        def _():
            first_start(q + AHEAD)

        @pl.when(q == CHUNKS - AHEAD)
        def _():
            other_slab(1).start()

        @pl.when(q == CHUNKS - 1)
        def _():
            own_slab(1).start()

        deep = pl.ds(pl.multiple_of(q * chunk, chunk), chunk)
        weights = jnp.concatenate([wv[1, deep, pl.ds(0, HALF)], wv[0, deep, pl.ds(HALF, HALF)]], axis=1)
        acc[...] += jnp.dot(xv[:, deep], weights, preferred_element_type=F32)
        return carry

    lax.fori_loop(0, CHUNKS, piece_of_depth, 0)
    for at in pieces:
        pbuf[0, at] = acc[at, :HALF].astype(BF16)
        own[at] = acc[at, HALF:].astype(BF16)

    other_slab(2).start()
    p_copy(0).start()
    other_slab(1).wait()
    other_product(1)

    def fence(t):
        p_copy(t - 1).wait()

        @pl.when(t >= LAG)
        def _():
            s_wait(t - LAG)

        send_chip(t - 1, 0)
        send_chip(t - 1, 1)
        p_copy(t).start()

        @pl.when(t >= LAG + 1)
        def _():
            y_copy(t - LAG - 1).start()

    def next_slabs(t):
        own_slab(t + 1).start()

        @pl.when(t + 2 < tiles)
        def _():
            other_slab(t + 2).start()

    def tile(t, carry):
        next_slabs(t)
        fence(t)
        own_slab(t).wait()
        other_slab(t + 1).wait()
        both = dot(xv[...], wv[lax.rem(t, 2)]).astype(BF16)
        pbuf[lax.rem(t + 1, 2)] = both[:, :HALF]
        own[...] = both[:, HALF:]
        sum_all(t - LAG)
        return carry

    def own_halves(t):
        own_slab(t).wait()
        own_product(t, 0)
        sum_all(t - LAG)
        p_copy(t).wait()
        send_chip(t, 0)
        own_product(t, 1)
        send_chip(t, 1)

    def split_tile(t, carry):
        next_slabs(t)
        own_halves(t)
        s_wait(t - 2)
        other_slab(t + 1).wait()
        other_product(t + 1)
        p_copy(t + 1).start()
        y_copy(t - LAG).start()
        return carry

    lax.fori_loop(1, tiles - SPLIT, tile, 0)
    fence(tiles - SPLIT)
    lax.fori_loop(tiles - SPLIT, last, split_tile, 0)
    own_halves(last)

    y_copy(last - LAG).start()
    for v in (last - 2, last - 1):
        s_wait(v)
        sum_all(v)
        y_copy(v).start()
    for h in range(2):
        s_copy(last, h).wait()
        sum_all(last, pieces[h * len(pieces) // 2 : (h + 1) * len(pieces) // 2])
        y_last(h).start()

    def finish(v, carry):
        y_copy(v).wait()
        return carry

    lax.fori_loop(0, last, finish, 0)
    for h in range(2):
        y_last(h).wait()


def place(y, out, sems):
    tiles = out.shape[1] // TILE
    copies = []
    for t in range(tiles):
        for h in range(2):
            copies.append(
                pltpu.make_async_copy(y.at[t + LAG, h], out.at[:, pl.ds(t * TILE + h * HALF, HALF)], sems.at[2 * t + h])
            )
    for c in copies:
        c.start()
    for c in copies:
        c.wait()


def solution(mesh):
    def local(x, w):
        rows, depth = x.shape
        columns = w.shape[1]
        tiles = columns // TILE
        x = pltpu.with_memory_space_constraint(x, pltpu.HBM)
        w = pltpu.with_memory_space_constraint(w, pltpu.HBM)
        y = pl.pallas_call(
            fused,
            out_shape=pltpu.VMEM((tiles + LAG, 2, rows, HALF), BF16),
            in_specs=[pl.BlockSpec(memory_space=pl.ANY)] * 2,
            out_specs=pl.BlockSpec(memory_space=pltpu.VMEM),
            scratch_shapes=[
                pltpu.VMEM((rows, depth), BF16),
                pltpu.VMEM((2, depth, TILE), BF16),
                pltpu.VMEM((rows, TILE), F32),
                pltpu.VMEM((rows, HALF), BF16),
                pltpu.VMEM((2, rows, HALF), BF16),
                pltpu.VMEM((2, rows, HALF), BF16),
                pltpu.VMEM((4, rows, HALF), BF16),
                pltpu.SemaphoreType.DMA((CHUNKS,)),
                pltpu.SemaphoreType.DMA((2, CHUNKS)),
                pltpu.SemaphoreType.DMA((2, 2)),
                pltpu.SemaphoreType.DMA((2,)),
                pltpu.SemaphoreType.DMA((2,)),
                pltpu.SemaphoreType.DMA((tiles, 2)),
                pltpu.SemaphoreType.DMA((tiles, 2)),
                pltpu.SemaphoreType.DMA((tiles + 1,)),
                pltpu.SemaphoreType.DMA((tiles + 1,)),
            ],
            compiler_params=pltpu.CompilerParams(
                collective_id=0, has_side_effects=True, vmem_limit_bytes=48 * 2**20
            ),
            name="fused",
        )(x, w)
        return pl.pallas_call(
            place,
            out_shape=jax.ShapeDtypeStruct((rows, columns), BF16),
            in_specs=[pl.BlockSpec(memory_space=pltpu.VMEM)],
            out_specs=pl.BlockSpec(memory_space=pl.ANY),
            scratch_shapes=[pltpu.SemaphoreType.DMA((2 * tiles,))],
            compiler_params=pltpu.CompilerParams(vmem_limit_bytes=16 * 2**20),
            name="place",
        )(y)

    return jax.shard_map(local, mesh=mesh, in_specs=(P("data", "tp"), P("tp", None)), out_specs=P("data", None), check_vma=False)
```
